32 devices in a mesh: gx: 4 (over z), gy: 8 (over y, x, core).
Axes of the slice: x: 2, y: 2, z: 4, core: 2. Of those that a mesh axis runs over, the one named last changes fastest.
Arguments:
- group_one: bfloat16 [6144, 768], P(('gx', 'gy')), may hold values from -6 to 6
- routes_one: int32 [6144, 1], P(('gx', 'gy')), may hold values from 0 to 31; in each aligned block of 192 rows (0 to 191, 192 to 383, ...) at most 6 rows name the same one
- gates_one: float32 [6144], P(('gx', 'gy')), may hold values from 0.2 to 1
- group_two: bfloat16 [6144, 768], P(('gx', 'gy')), may hold values from -6 to 6
- routes_two: int32 [6144, 1], P(('gx', 'gy')), may hold values from 0 to 31; in each aligned block of 192 rows (0 to 191, 192 to 383, ...) at most 6 rows name the same one
- gates_two: float32 [6144], P(('gx', 'gy')), may hold values from 0.2 to 1
- norm_gain: float32 [768], replicated, may hold values from 0.1 to 1.9
- weight_in: bfloat16 [32, 768, 3072], P(('gx', 'gy')), may hold values from -0.21875 to 0.21875
- weight_out: bfloat16 [32, 3072, 768], P(('gx', 'gy')), may hold values from -0.109375 to 0.109375
- old_place: int32 [32], replicated, may hold values from 0 to 31, each once
- partner: int32 [32], replicated, may hold values from 0 to 31, as said below
Outputs:
- result_one: bfloat16 [6144, 768], P(('gx', 'gy'))
- result_two: bfloat16 [6144, 768], P(('gx', 'gy'))
- new_in: bfloat16 [32, 768, 3072], P(('gx', 'gy'))
- new_out: bfloat16 [32, 3072, 768], P(('gx', 'gy'))
The draws below stay inside these ranges and needn't reach their ends.
Inputs may be any that keep to these rules, and one draw needn't show every extreme that they name: `routes_one`: at most 6 tokens of one device's rows in a block name the same expert, a bound that some block reaches of some device's rows in every draw. `routes_two`: same law as routes_one. partner is an involution: partner[partner[s]] = s; exactly 16 slots have partner[s] != s.
All inputs are finite; a program needn't handle non-finite values.
Results may differ from the reference program's by a relative error of at most 0.0041.
Values may be sent and summed in bfloat16 or wider, within the bound.
A program may use at most 128 MiB of HBM per device.

```python
import math
import jax
import jax.numpy as jnp
import numpy as np
from jax import lax

D = 768
FF = 3072
TOK_DEV = 192
CAP = 6
EXPERTS = 32
TOKENS = 6144
EXPERT_ROWS = 192


def draw_partner(key, part):
    shuffled = jax.random.permutation(jax.random.fold_in(key, 7), EXPERTS).astype(jnp.int32)
    moved = EXPERTS // 2
    givers = shuffled[0:moved:2]
    takers = shuffled[1:moved:2]
    labels = jnp.arange(EXPERTS, dtype=jnp.int32)
    return labels.at[givers].set(takers).at[takers].set(givers)


def steps_of(stream_key, extent, split, low, top_value):
    factor_of, own = 1.0, jax.random.fold_in(stream_key, 6)
    for dim, blocks in split:
        heights = jnp.exp(jax.random.uniform(jax.random.fold_in(own, dim), (blocks,), jnp.float32, low / len(split), top_value / len(split)))
        factor_of = factor_of * jnp.repeat(heights, extent[dim] // blocks).reshape([-1 if axis == dim else 1 for axis in range(len(extent))])
    return factor_of


def shared_out(own_key, own, number, rows, count, top, limit, slope):
    sequence = jax.random.permutation(own_key, count)
    heavy_load, common = portions_of(count, rows * top, limit, slope, True), portions_of(count, rows * top, limit, slope, False)
    places = jnp.arange(count)

    def named(lengths, offset_by):
        used = int((lengths > 0).sum())
        fixed = max(1, used // 4)
        shifted = fixed + (places - fixed + offset_by * (used - fixed)) % max(1, count - fixed)
        return jnp.zeros((count,), jnp.int32).at[sequence[jnp.where(places < fixed, places, shifted)]].set(jnp.asarray(lengths, jnp.int32))

    lengths = jnp.where(number % 4 == 0, named(heavy_load, number // 4), named(common, number - number // 4 - 1))
    mixed = jax.random.permutation(jax.random.fold_in(own, 3), count)
    giver, taker = mixed[0:count // 2 * 2:2], mixed[1:count // 2 * 2:2]
    margin = jnp.minimum(lengths[giver] - 1, limit - lengths[taker]) // 2
    margin = jnp.where((giver == sequence[0]) | (taker == sequence[0]) | (lengths[taker] == 0), 0, jnp.maximum(margin, 0))
    shifted = jax.random.randint(jax.random.fold_in(own, 4), (count // 2,), 0, 1 << 20) % (margin + 1)
    lengths = lengths.at[giver].add(-shifted).at[taker].add(shifted)
    items = jnp.searchsorted(jnp.cumsum(lengths), jnp.arange(rows * top), side="right").astype(jnp.int32)
    table = items.reshape(top, rows).T
    table = table[jax.random.permutation(jax.random.fold_in(own, 1), rows)]
    offset_by = jax.random.randint(jax.random.fold_in(own, 2), (rows, 1), 0, top)
    return jnp.take_along_axis(table, (jnp.arange(top)[None, :] + offset_by) % top, axis=1)


def portions_of(number_of, total, bound, lean, full):
    weights = [(1 << 20) // math.isqrt(grade ** lean) + 1 for grade in range(1, number_of + 1)]
    largest = bound if full else min(bound, max(-(-total // number_of), total * weights[0] // sum(weights)))
    least = 1 if total - largest >= number_of - 1 else 0
    given, spare = [largest] + [least] * (number_of - 1), total - largest - least * (number_of - 1)
    while spare > 0:
        free = [i for i in range(1, number_of) if given[i] < largest] or [i for i in range(1, number_of) if given[i] < bound]
        whole, remaining = sum([weights[i] for i in free]), spare
        for i in free:
            extra = min(bound - given[i], max(1, remaining * weights[i] // whole), spare)
            given[i] = given[i] + extra
            spare = spare - extra
    return np.array(given)


def centred(rng, extent, width, most, cuts=(), kind=jnp.bfloat16):
    drawn = width * jax.random.normal(rng, extent, jnp.float32)
    if cuts:
        drawn = drawn * steps_of(rng, extent, cuts, -0.22, 0.18)
    return jnp.clip(drawn, -most, most).astype(kind)


def setup_inputs(seed: int = 0) -> dict:
    arg_keys = jax.random.split(jax.random.key(seed), 12)
    group_one = centred(arg_keys[0], (TOKENS, D), 1.0, 6.0, ((0, 32),))
    routes_one_keys = jax.random.split(jax.random.fold_in(arg_keys[1], 1), TOKENS // TOK_DEV)
    routes_one_turns = jax.random.permutation(jax.random.fold_in(arg_keys[1], 3), TOKENS // TOK_DEV)
    routes_one = jax.vmap(lambda own, number: shared_out(jax.random.fold_in(arg_keys[1], 2), own, number, TOK_DEV, EXPERTS, 1, CAP, 2))(routes_one_keys, routes_one_turns).reshape((TOKENS, 1))
    gates_one = jnp.clip(0.2 + 0.8 * jax.random.uniform(arg_keys[2], (TOKENS,), jnp.float32) ** steps_of(arg_keys[2], (TOKENS,), ((0, 32),), -0.2, 0.2), 0.2, 1.0)
    group_two = centred(arg_keys[3], (TOKENS, D), 1.0, 6.0, ((0, 32),))
    routes_two_keys = jax.random.split(jax.random.fold_in(arg_keys[4], 1), TOKENS // TOK_DEV)
    routes_two_turns = jax.random.permutation(jax.random.fold_in(arg_keys[4], 3), TOKENS // TOK_DEV)
    routes_two = jax.vmap(lambda own, number: shared_out(jax.random.fold_in(arg_keys[4], 2), own, number, TOK_DEV, EXPERTS, 1, CAP, 2))(routes_two_keys, routes_two_turns).reshape((TOKENS, 1))
    gates_two = jnp.clip(0.2 + 0.8 * jax.random.uniform(arg_keys[5], (TOKENS,), jnp.float32) ** steps_of(arg_keys[5], (TOKENS,), ((0, 32),), -0.2, 0.2), 0.2, 1.0)
    norm_gain = jnp.clip(1.0 + 0.18 * jax.random.normal(arg_keys[6], (D,), jnp.float32), 0.1, 1.9)
    weight_in = centred(arg_keys[7], (EXPERTS, D, FF), D ** -0.5, 0.21875, ((0, 32),))
    weight_out = centred(arg_keys[8], (EXPERTS, FF, D), FF ** -0.5, 0.109375, ((0, 32),))
    old_place = jax.random.permutation(arg_keys[9], EXPERTS).astype(jnp.int32)
    partner = draw_partner(jax.random.fold_in(arg_keys[11], 71), 0)
    return {"group_one": group_one, "routes_one": routes_one, "gates_one": gates_one, "group_two": group_two, "routes_two": routes_two, "gates_two": gates_two, "norm_gain": norm_gain, "weight_in": weight_in, "weight_out": weight_out, "old_place": old_place, "partner": partner}


epsilon = 1e-06

def expert_table(routes):
    expert_ids = routes[:, 0].astype(jnp.int32)
    ordering = jnp.argsort(expert_ids, stable=True).astype(jnp.int32)
    sorted_ids = expert_ids[ordering]
    counts = jnp.zeros((EXPERTS,), jnp.int32).at[expert_ids].add(1)
    starts = jnp.cumsum(counts).astype(jnp.int32) - counts
    placed = jnp.arange(TOKENS, dtype=jnp.int32) - starts[sorted_ids]
    row_table = jnp.full((EXPERTS, EXPERT_ROWS), TOKENS, jnp.int32)
    return row_table.at[sorted_ids, placed].set(ordering)

def switch_layer(tokens_in, routes, gate_probs, norm_gain, weight_in, weight_out, holder):
    values = tokens_in.astype(jnp.float32)
    scaling = lax.rsqrt(lax.optimization_barrier(jnp.mean(values * values, axis=1, keepdims=True)) + epsilon)
    normed = (values * scaling * norm_gain.astype(jnp.float32)).astype(jnp.bfloat16)
    padded = jnp.concatenate([normed, jnp.zeros((1, D), jnp.bfloat16)], axis=0)
    row_table = expert_table(routes)

    def one_expert(members):
        entries, holder_slot = members
        inputs = padded[entries]
        hidden = jnp.maximum(jnp.dot(inputs, weight_in[holder_slot], preferred_element_type=jnp.float32), 0.0).astype(jnp.bfloat16)
        return jnp.dot(hidden, weight_out[holder_slot], preferred_element_type=jnp.float32).astype(jnp.bfloat16)
    outputs = lax.map(one_expert, (row_table, holder))
    gathered = jnp.zeros((TOKENS + 1, D), jnp.bfloat16).at[row_table].set(outputs)[:TOKENS]
    mixed = values + gate_probs.astype(jnp.float32)[:, None] * gathered.astype(jnp.float32)
    return mixed.astype(jnp.bfloat16)

def reference(group_one, routes_one, gates_one, group_two, routes_two, gates_two, norm_gain, weight_in, weight_out, old_place, partner):
    holder = jnp.argsort(old_place).astype(jnp.int32)
    first_out = switch_layer(group_one, routes_one, gates_one, norm_gain, weight_in, weight_out, holder)
    second = switch_layer(group_two, routes_two, gates_two, norm_gain, weight_in, weight_out, holder)
    new_in = jnp.take(weight_in, partner, axis=0)
    new_out = jnp.take(weight_out, partner, axis=0)
    return (first_out, second, new_in, new_out)
```

```python
import jax
import jax.numpy as jnp
from jax import lax
from jax.experimental import pallas as pl
from jax.experimental.pallas import tpu as pltpu
from jax.sharding import PartitionSpec as P

CAP = 6
AXES = ("gx", "gy")

epsilon = 1e-06


def rows_of(table, keys):
    labels = lax.iota(jnp.int32, table.shape[0])
    return jnp.sum(jnp.where(keys[:, None] == labels[None, :], table[None, :], 0), axis=1)


MESH = pl.DeviceIdType.MESH
PARTS = 6
NARROW = 6


def planes_of(partner, cap):
    planes, width = lax.axis_size("gx"), lax.axis_size("gy")
    slots = planes * width
    here = lax.axis_index("gx")
    labels = lax.iota(jnp.int32, slots)
    plane = labels // width
    half = labels // (2 * width)
    goal_plane, goal_half = partner // width, partner // (2 * width)
    leaves = goal_plane != plane
    crosses = goal_half != half
    earlier = labels[None, :] < labels[:, None]
    same_plane = plane[None, :] == plane[:, None]
    same_half = half[None, :] == half[:, None]
    rank_plane = jnp.sum(jnp.where(earlier & same_plane & leaves[None, :], 1, 0), axis=1)
    rank_half = jnp.sum(jnp.where(earlier & same_half & crosses[None, :], 1, 0), axis=1)
    outer = (here == 0) | (here == planes - 1)
    order = lax.iota(jnp.int32, cap)

    def listed(member, rank, code):
        hit = member[None, :] & (rank[None, :] == order[:, None])
        return jnp.sum(jnp.where(hit, code[None, :], 0), axis=1)

    my_half = here // 2
    first = jnp.where(plane == here, labels % width, 16 + rank_plane)
    forward = listed(
        jnp.where(outer, leaves & (plane == here), crosses & (half == my_half)),
        jnp.where(outer, rank_plane, rank_half),
        first,
    )
    edge = jnp.where(here == 1, 0, planes - 1)
    code = jnp.where(goal_plane == here, partner % width, 32 + rows_of(rank_half, partner))
    backward = listed(leaves & (plane == edge), rank_plane, code)
    far = jnp.where(
        outer,
        16 + rank_plane,
        jnp.where(
            goal_half == my_half,
            16 + rows_of(rank_plane, partner),
            32 + rows_of(rank_half, partner),
        ),
    )
    final = jnp.where(goal_plane == here, partner % width, far)
    final = lax.dynamic_slice(final, (here * width,), (width,))
    return jnp.concatenate([forward, backward, final])


def crossing_count(partner):
    planes, width = lax.axis_size("gx"), lax.axis_size("gy")
    labels = lax.iota(jnp.int32, planes * width)
    plane, goal = labels // width, partner // width
    counts = [
        jnp.sum(jnp.where((plane <= cut) & (goal > cut), 1, 0)) for cut in range(planes - 1)
    ]
    return jnp.maximum(jnp.maximum(counts[0], counts[1]), counts[2])


def relocate_kernel(cap, width, tab, w_in, w_out, o_in, o_out, *scr):
    weights, outs = (w_in, w_out), (o_in, o_out)
    chunks = 2 * PARTS
    groups = [scr[i * chunks : (i + 1) * chunks] for i in range(6)]
    own, near, across, ahead, behind, ready = groups
    (own_sem, near_sem, across_sem, spread_sem, ahead_sem, behind_sem, ready_sem, out_sem) = scr[
        6 * chunks :
    ]
    gx, gy = lax.axis_index("gx"), lax.axis_index("gy")
    planes = 4
    outer = (gx == 0) | (gx == planes - 1)
    inner = jnp.where(gx == 0, 1, 2)
    edge = jnp.where(gx == 1, 0, 3)
    other = jnp.where(gx == 1, 2, 1)

    def rows(c, piece):
        step = weights[c // PARTS].shape[1] // (width * PARTS)
        start = piece * (step * PARTS) + (c % PARTS) * step
        return pl.ds(pl.multiple_of(start, step), step)

    barrier = pltpu.get_barrier_semaphore()
    for r in range(1, width):
        pl.semaphore_signal(
            barrier, inc=1, device_id=(gx, jnp.bitwise_xor(gy, r)), device_id_type=MESH
        )

    @pl.when(outer)
    def _():
        pl.semaphore_signal(barrier, inc=1, device_id=(inner, gy), device_id_type=MESH)
        pl.semaphore_wait(barrier, width)

    @pl.when(jnp.logical_not(outer))
    def _():
        pl.semaphore_signal(barrier, inc=1, device_id=(edge, gy), device_id_type=MESH)
        pl.semaphore_signal(barrier, inc=1, device_id=(other, gy), device_id_type=MESH)
        pl.semaphore_wait(barrier, width + 1)

    for c in range(chunks):
        weight = weights[c // PARTS]
        for r in range(1, width):
            target = jnp.bitwise_xor(gy, r)
            pltpu.make_async_remote_copy(
                src_ref=weight.at[0, rows(c, target)],
                dst_ref=own[c].at[gy],
                send_sem=spread_sem.at[c],
                recv_sem=own_sem.at[c],
                device_id=(gx, target),
                device_id_type=MESH,
            ).start()
        pltpu.make_async_copy(weight.at[0, rows(c, gy)], own[c].at[gy], own_sem.at[c]).start()

    def fill(c, dest, base, count, sources):
        ref = dest[c]
        columns = ref.shape[2]
        tall = ref.shape[1]

        def one(i, carry):
            code = tab[base + i]
            kind, index = code // 16, code % 16
            for part in range(4):
                if tall == 16:
                    at = (slice(None), pl.ds(part * (columns // 4), columns // 4))
                else:
                    at = (pl.ds(part * (tall // 4), tall // 4), slice(None))
                value = None
                for number, source in sources:
                    loaded = source[c][jnp.where(kind == number, index, 0), at[0], at[1]]
                    value = loaded if value is None else jnp.where(kind == number, loaded, value)
                ref[i, at[0], at[1]] = value
            return carry

        lax.fori_loop(0, count, one, 0)

    def send(c, source, target, dest, send_sem, recv_sem):
        pltpu.make_async_remote_copy(
            src_ref=source[c],
            dst_ref=dest[c],
            send_sem=send_sem.at[c],
            recv_sem=recv_sem.at[c],
            device_id=(target, gy),
            device_id_type=MESH,
        ).start()

    def arrived(buffer, sem, c):
        pltpu.make_async_copy(buffer[c], buffer[c], sem.at[c]).wait()

    def collect(c, sources):
        fill(c, ready, 2 * cap, width, sources)
        out = outs[c // PARTS]
        for r in range(1, width):
            target = jnp.bitwise_xor(gy, r)
            pltpu.make_async_remote_copy(
                src_ref=ready[c].at[target],
                dst_ref=out.at[0, rows(c, gy)],
                send_sem=ready_sem.at[c],
                recv_sem=out_sem.at[c // PARTS],
                device_id=(gx, target),
                device_id_type=MESH,
            ).start()
        pltpu.make_async_copy(
            ready[c].at[gy], out.at[0, rows(c, gy)], out_sem.at[c // PARTS]
        ).start()

    @pl.when(outer)
    def _():
        lag = 3
        for t in range(chunks + lag):
            if t < chunks:
                arrived(own, own_sem, t)
                fill(t, ahead, 0, cap, ((0, own),))
                send(t, ahead, inner, near, ahead_sem, near_sem)
            c = t - lag
            if c >= 0:
                arrived(near, near_sem, c)
                collect(c, ((0, own), (1, near)))

    @pl.when(jnp.logical_not(outer))
    def _():
        for t in range(chunks + 1):
            if t < chunks:
                arrived(own, own_sem, t)
                arrived(near, near_sem, t)
                fill(t, ahead, 0, cap, ((0, own), (1, near)))
                send(t, ahead, other, across, ahead_sem, across_sem)
            c = t - 1
            if c >= 0:
                arrived(across, across_sem, c)
                fill(c, behind, cap, cap, ((0, own), (2, across)))
                send(c, behind, edge, near, behind_sem, near_sem)
                collect(c, ((0, own), (1, near), (2, across)))

    for number in range(2):
        pltpu.make_async_copy(outs[number], outs[number], out_sem.at[number]).wait()
    for c in range(chunks):
        seven = own[c].at[pl.ds(0, width - 1)]
        pltpu.make_async_copy(seven, seven, spread_sem.at[c]).wait()
        pltpu.make_async_copy(seven, seven, ready_sem.at[c]).wait()
        pltpu.make_async_copy(ahead[c], ahead[c], ahead_sem.at[c]).wait()

    @pl.when(jnp.logical_not(outer))
    def _():
        for c in range(chunks):
            pltpu.make_async_copy(behind[c], behind[c], behind_sem.at[c]).wait()


def relocate_planes(cap, number, weight_in, weight_out, partner):
    width = lax.axis_size("gy")
    chunks = 2 * PARTS

    def buffers(slots):
        kinds = []
        for weight in (weight_in, weight_out):
            _, tall, columns = weight.shape
            kinds += [pltpu.VMEM((slots, tall // (width * PARTS), columns), weight.dtype)] * PARTS
        return kinds

    scratch = buffers(width) + buffers(cap) * 4 + buffers(width)
    scratch += [pltpu.SemaphoreType.DMA((chunks,))] * 7 + [pltpu.SemaphoreType.DMA((2,))]
    anywhere = pl.BlockSpec(memory_space=pl.ANY)
    return pl.pallas_call(
        lambda *refs: relocate_kernel(cap, width, *refs),
        out_shape=(
            jax.ShapeDtypeStruct(weight_in.shape, weight_in.dtype),
            jax.ShapeDtypeStruct(weight_out.shape, weight_out.dtype),
        ),
        in_specs=[pl.BlockSpec(memory_space=pltpu.SMEM), anywhere, anywhere],
        out_specs=(anywhere, anywhere),
        scratch_shapes=scratch,
        compiler_params=pltpu.CompilerParams(
            collective_id=number, has_side_effects=True, vmem_limit_bytes=64 * 1024 * 1024 - 65536
        ),
        name="relocate",
    )(planes_of(partner, cap), weight_in, weight_out)


def relocate_by_planes(weight_in, weight_out, partner):
    width = lax.axis_size("gy")
    return lax.cond(
        crossing_count(partner) <= NARROW,
        lambda a, b, p: relocate_planes(NARROW, 0, a, b, p),
        lambda a, b, p: relocate_planes(width, 1, a, b, p),
        weight_in,
        weight_out,
        partner,
    )


def relocate_flat(weight_in, weight_out, partner):
    devices = lax.axis_size(AXES)
    stacked = jnp.stack([weight_in.reshape(devices, -1), weight_out.reshape(devices, -1)], axis=1)
    pieces = lax.all_to_all(stacked, AXES, split_axis=0, concat_axis=0, tiled=True)
    reordered = jnp.take(pieces, partner, axis=0)
    settled = lax.all_to_all(reordered, AXES, split_axis=0, concat_axis=0, tiled=True)
    return (settled[:, 0].reshape(weight_in.shape), settled[:, 1].reshape(weight_out.shape))


def both_blocks(groups, routes, gates, norm_gain, old_place, weight_in, weight_out):
    devices = lax.axis_size(AXES)
    rows, model_width = groups[0].shape
    slots = lax.iota(jnp.int32, devices)
    places = []
    lower = (
        lax.broadcasted_iota(jnp.int32, (rows, rows), 0)
        > lax.broadcasted_iota(jnp.int32, (rows, rows), 1)
    ).astype(jnp.bfloat16)
    for block, names in enumerate(routes):
        member = names == old_place[None, :]
        before = jnp.dot(lower, member.astype(jnp.bfloat16), preferred_element_type=jnp.float32)
        spot = slots[None, :] * (2 * CAP) + block * CAP + before.astype(jnp.int32)
        places.append(jnp.sum(jnp.where(member, spot, 0), axis=1))
    place = jnp.concatenate(places)
    total = devices * 2 * CAP
    values = jnp.concatenate(groups, axis=0).astype(jnp.float32)
    scaling = lax.rsqrt(jnp.mean(values * values, axis=1, keepdims=True) + epsilon)
    normed = (values * scaling * norm_gain).astype(jnp.bfloat16)
    chosen = (lax.iota(jnp.int32, total)[:, None] == place[None, :]).astype(jnp.bfloat16)
    outgoing = jnp.dot(chosen, normed, preferred_element_type=jnp.float32).astype(jnp.bfloat16)
    arrived = lax.all_to_all(
        outgoing.reshape(devices, 2 * CAP, model_width), AXES, split_axis=0, concat_axis=0, tiled=True
    ).reshape(total, model_width)
    hidden = jnp.maximum(
        jnp.dot(arrived, weight_in[0], preferred_element_type=jnp.float32), 0.0
    ).astype(jnp.bfloat16)
    result = jnp.dot(hidden, weight_out[0], preferred_element_type=jnp.float32).astype(jnp.bfloat16)
    returned = lax.all_to_all(
        result.reshape(devices, 2 * CAP, model_width), AXES, split_axis=0, concat_axis=0, tiled=True
    ).reshape(total, model_width)
    answer = lax.dot_general(
        chosen, returned, (((0,), (0,)), ((), ())), preferred_element_type=jnp.float32
    )
    gate = jnp.concatenate(gates)[:, None]
    mixed = (values + gate * answer).astype(jnp.bfloat16)
    return mixed[:rows], mixed[rows:]


def local(
    group_one,
    routes_one,
    gates_one,
    group_two,
    routes_two,
    gates_two,
    norm_gain,
    weight_in,
    weight_out,
    old_place,
    partner,
):
    first, second = both_blocks(
        (group_one, group_two),
        (routes_one, routes_two),
        (gates_one, gates_two),
        norm_gain,
        old_place,
        weight_in,
        weight_out,
    )
    by_planes = (lax.axis_size("gx"), lax.axis_size("gy")) == (4, 8)
    relocate = relocate_by_planes if by_planes else relocate_flat
    new_in, new_out = relocate(weight_in, weight_out, partner)
    return (first, second, new_in, new_out)


def solution(mesh):
    split = ("gx", "gy")
    rows, flat, cube = P(split, None), P(split), P(split, None, None)
    return jax.shard_map(
        local,
        mesh=mesh,
        in_specs=(rows, rows, flat, rows, rows, flat, P(), cube, cube, P(), P()),
        out_specs=(rows, rows, cube, cube),
        check_vma=False,
    )
```

```python
import functools

import jax
import jax.numpy as jnp
from jax import lax
from jax.experimental import pallas as pl
from jax.experimental.pallas import tpu as pltpu
from jax.sharding import PartitionSpec as P

CAP = 6
AXES = ("gx", "gy")

epsilon = 1e-06


def rows_of(table, keys):
    labels = lax.iota(jnp.int32, table.shape[0])
    return jnp.sum(jnp.where(keys[:, None] == labels[None, :], table[None, :], 0), axis=1)


MESH = pl.DeviceIdType.MESH
PARTS = 6
NARROW = (5, 6)
SEAT = 16
TILE = 256


def planes_of(partner, cap):
    planes, width = lax.axis_size("gx"), lax.axis_size("gy")
    slots = planes * width
    here = lax.axis_index("gx")
    labels = lax.iota(jnp.int32, slots)
    plane = labels // width
    half = labels // (2 * width)
    goal_plane, goal_half = partner // width, partner // (2 * width)
    leaves = goal_plane != plane
    crosses = goal_half != half
    earlier = labels[None, :] < labels[:, None]
    same_plane = plane[None, :] == plane[:, None]
    same_half = half[None, :] == half[:, None]
    rank_plane = jnp.sum(jnp.where(earlier & same_plane & leaves[None, :], 1, 0), axis=1)
    rank_half = jnp.sum(jnp.where(earlier & same_half & crosses[None, :], 1, 0), axis=1)
    outer = (here == 0) | (here == planes - 1)
    order = lax.iota(jnp.int32, cap)

    def listed(member, rank, code):
        hit = member[None, :] & (rank[None, :] == order[:, None])
        return jnp.sum(jnp.where(hit, code[None, :], 0), axis=1)

    my_half = here // 2
    first = jnp.where(plane == here, labels % width, 16 + rank_plane)
    forward = listed(
        jnp.where(outer, leaves & (plane == here), crosses & (half == my_half)),
        jnp.where(outer, rank_plane, rank_half),
        first,
    )
    edge = jnp.where(here == 1, 0, planes - 1)
    code = jnp.where(goal_plane == here, partner % width, 32 + rows_of(rank_half, partner))
    backward = listed(leaves & (plane == edge), rank_plane, code)
    far = jnp.where(
        outer,
        16 + rank_plane,
        jnp.where(
            goal_half == my_half,
            16 + rows_of(rank_plane, partner),
            32 + rows_of(rank_half, partner),
        ),
    )
    final = jnp.where(goal_plane == here, partner % width, far)
    final = lax.dynamic_slice(final, (here * width,), (width,))
    return jnp.concatenate([forward, backward, final])


def crossing_count(partner):
    planes, width = lax.axis_size("gx"), lax.axis_size("gy")
    labels = lax.iota(jnp.int32, planes * width)
    plane, goal = labels // width, partner // width
    counts = [
        jnp.sum(jnp.where((plane <= cut) & (goal > cut), 1, 0)) for cut in range(planes - 1)
    ]
    return jnp.maximum(jnp.maximum(counts[0], counts[1]), counts[2])


def relocate_kernel(cap, width, tab, w_in, w_out, sent, o_in, o_out, returned, *scr):
    weights, outs = (w_in, w_out), (o_in, o_out)
    chunks = 2 * PARTS
    groups = [scr[i * chunks : (i + 1) * chunks] for i in range(6)]
    own, near, across, ahead, behind, ready = groups
    (own_sem, near_sem, across_sem, spread_sem, ahead_sem, behind_sem, ready_sem, out_sem) = scr[
        6 * chunks : 6 * chunks + 8
    ]
    inbox, reply, total, tile_in, tile_out, token_sem, tile_sem = scr[6 * chunks + 8 :]
    gx, gy = lax.axis_index("gx"), lax.axis_index("gy")
    planes = 4
    outer = (gx == 0) | (gx == planes - 1)
    inner = jnp.where(gx == 0, 1, 2)
    edge = jnp.where(gx == 1, 0, 3)
    other = jnp.where(gx == 1, 2, 1)

    def rows(c, piece):
        step = weights[c // PARTS].shape[1] // (width * PARTS)
        start = piece * (step * PARTS) + (c % PARTS) * step
        return pl.ds(pl.multiple_of(start, step), step)

    me = gx * width + gy
    peers = []
    for a in range(planes):
        for b in range(width):
            if a or b:
                peers.append((jnp.bitwise_xor(gx, a), jnp.bitwise_xor(gy, b)))

    barrier = pltpu.get_barrier_semaphore()
    for peer in peers:
        pl.semaphore_signal(barrier, inc=1, device_id=peer, device_id_type=MESH)
    pl.semaphore_wait(barrier, len(peers))

    def to_all(source, dest, send_sem, recv_sem):
        for x, y in peers:
            pltpu.make_async_remote_copy(
                src_ref=source.at[x * width + y],
                dst_ref=dest.at[me],
                send_sem=send_sem,
                recv_sem=recv_sem,
                device_id=(x, y),
                device_id_type=MESH,
            ).start()
        pltpu.make_async_copy(source.at[me], dest.at[me], recv_sem).start()

    def all_here(ref, sem):
        pltpu.make_async_copy(ref, ref, sem).wait()

    to_all(sent, inbox, token_sem.at[0], token_sem.at[1])

    tiles = w_in.shape[2] // TILE

    def tile_copies(f, slot):
        at = pl.ds(pl.multiple_of(f * TILE, TILE), TILE)
        return (
            pltpu.make_async_copy(w_in.at[0, :, at], tile_in.at[slot], tile_sem.at[0, slot]),
            pltpu.make_async_copy(w_out.at[0, at, :], tile_out.at[slot], tile_sem.at[1, slot]),
        )

    for copy in tile_copies(0, 0):
        copy.start()

    def expert():
        all_here(inbox, token_sem.at[1])
        seats, seat, model = inbox.shape
        half = seats // 2
        total[...] = jnp.zeros_like(total)

        def one(f, carry):
            slot = f % 2
            for copy in tile_copies(f, slot):
                copy.wait()

            @pl.when(f + 1 < tiles)
            def _():
                for copy in tile_copies(f + 1, 1 - slot):
                    copy.start()

            for m in range(2):
                rows_here = pl.ds(m * half * seat, half * seat)
                tokens = inbox[pl.ds(m * half, half)].reshape(half * seat, model)
                hidden = jnp.dot(tokens, tile_in[slot], preferred_element_type=jnp.float32)
                hidden = jnp.maximum(hidden, 0.0).astype(jnp.bfloat16)
                total[rows_here, :] += jnp.dot(
                    hidden, tile_out[slot], preferred_element_type=jnp.float32
                )
            return carry

        lax.fori_loop(0, tiles, one, 0)
        reply[...] = total[...].astype(jnp.bfloat16).reshape(seats, seat, model)
        to_all(reply, returned, token_sem.at[2], token_sem.at[3])

    for c in range(chunks):
        weight = weights[c // PARTS]
        for r in range(1, width):
            target = jnp.bitwise_xor(gy, r)
            pltpu.make_async_remote_copy(
                src_ref=weight.at[0, rows(c, target)],
                dst_ref=own[c].at[gy],
                send_sem=spread_sem.at[c],
                recv_sem=own_sem.at[c],
                device_id=(gx, target),
                device_id_type=MESH,
            ).start()
        pltpu.make_async_copy(weight.at[0, rows(c, gy)], own[c].at[gy], own_sem.at[c]).start()

    def fill(c, dest, base, count, sources):
        ref = dest[c]
        columns = ref.shape[2]
        tall = ref.shape[1]

        def one(i, carry):
            code = tab[base + i]
            kind, index = code // 16, code % 16
            for part in range(4):
                if tall == 16:
                    at = (slice(None), pl.ds(part * (columns // 4), columns // 4))
                else:
                    at = (pl.ds(part * (tall // 4), tall // 4), slice(None))
                value = None
                for number, source in sources:
                    loaded = source[c][jnp.where(kind == number, index, 0), at[0], at[1]]
                    value = loaded if value is None else jnp.where(kind == number, loaded, value)
                ref[i, at[0], at[1]] = value
            return carry

        lax.fori_loop(0, count, one, 0)

    def send(c, source, target, dest, send_sem, recv_sem):
        pltpu.make_async_remote_copy(
            src_ref=source[c],
            dst_ref=dest[c],
            send_sem=send_sem.at[c],
            recv_sem=recv_sem.at[c],
            device_id=(target, gy),
            device_id_type=MESH,
        ).start()

    def arrived(buffer, sem, c):
        pltpu.make_async_copy(buffer[c], buffer[c], sem.at[c]).wait()

    def collect(c, sources):
        fill(c, ready, 2 * cap, width, sources)
        out = outs[c // PARTS]
        for r in range(1, width):
            target = jnp.bitwise_xor(gy, r)
            pltpu.make_async_remote_copy(
                src_ref=ready[c].at[target],
                dst_ref=out.at[0, rows(c, gy)],
                send_sem=ready_sem.at[c],
                recv_sem=out_sem.at[c // PARTS],
                device_id=(gx, target),
                device_id_type=MESH,
            ).start()
        pltpu.make_async_copy(
            ready[c].at[gy], out.at[0, rows(c, gy)], out_sem.at[c // PARTS]
        ).start()

    @pl.when(outer)
    def _():
        lag = 3
        for t in range(chunks + lag):
            if t < chunks:
                arrived(own, own_sem, t)
                fill(t, ahead, 0, cap, ((0, own),))
                send(t, ahead, inner, near, ahead_sem, near_sem)
            if t == 2:
                expert()
            c = t - lag
            if c >= 0:
                arrived(near, near_sem, c)
                collect(c, ((0, own), (1, near)))

    @pl.when(jnp.logical_not(outer))
    def _():
        for t in range(chunks + 1):
            if t < chunks:
                arrived(own, own_sem, t)
                arrived(near, near_sem, t)
                fill(t, ahead, 0, cap, ((0, own), (1, near)))
                send(t, ahead, other, across, ahead_sem, across_sem)
            if t == 0:
                expert()
            c = t - 1
            if c >= 0:
                arrived(across, across_sem, c)
                fill(c, behind, cap, cap, ((0, own), (2, across)))
                send(c, behind, edge, near, behind_sem, near_sem)
                collect(c, ((0, own), (1, near), (2, across)))

    all_here(returned, token_sem.at[3])
    others = inbox.at[pl.ds(0, len(peers))]
    all_here(others, token_sem.at[0])
    all_here(others, token_sem.at[2])
    for number in range(2):
        all_here(outs[number], out_sem.at[number])
    for c in range(chunks):
        seven = own[c].at[pl.ds(0, width - 1)]
        pltpu.make_async_copy(seven, seven, spread_sem.at[c]).wait()
        pltpu.make_async_copy(seven, seven, ready_sem.at[c]).wait()
        pltpu.make_async_copy(ahead[c], ahead[c], ahead_sem.at[c]).wait()

    @pl.when(jnp.logical_not(outer))
    def _():
        for c in range(chunks):
            pltpu.make_async_copy(behind[c], behind[c], behind_sem.at[c]).wait()


def relocate_planes(cap, number, weight_in, weight_out, sent, partner):
    width = lax.axis_size("gy")
    chunks = 2 * PARTS

    def buffers(slots):
        kinds = []
        for weight in (weight_in, weight_out):
            _, tall, columns = weight.shape
            kinds += [pltpu.VMEM((slots, tall // (width * PARTS), columns), weight.dtype)] * PARTS
        return kinds

    scratch = buffers(width) + buffers(cap) * 4 + buffers(width)
    scratch += [pltpu.SemaphoreType.DMA((chunks,))] * 7 + [pltpu.SemaphoreType.DMA((2,))]
    model, inside = weight_in.shape[1:]
    scratch += [
        pltpu.VMEM(sent.shape, sent.dtype),
        pltpu.VMEM(sent.shape, sent.dtype),
        pltpu.VMEM((sent.shape[0] * sent.shape[1], model), jnp.float32),
        pltpu.VMEM((2, model, TILE), weight_in.dtype),
        pltpu.VMEM((2, TILE, model), weight_in.dtype),
        pltpu.SemaphoreType.DMA((4,)),
        pltpu.SemaphoreType.DMA((2, 2)),
    ]
    anywhere = pl.BlockSpec(memory_space=pl.ANY)
    return pl.pallas_call(
        lambda *refs: relocate_kernel(cap, width, *refs),
        out_shape=(
            jax.ShapeDtypeStruct(weight_in.shape, weight_in.dtype),
            jax.ShapeDtypeStruct(weight_out.shape, weight_out.dtype),
            jax.ShapeDtypeStruct(sent.shape, sent.dtype),
        ),
        in_specs=[pl.BlockSpec(memory_space=pltpu.SMEM), anywhere, anywhere, anywhere],
        out_specs=(anywhere, anywhere, anywhere),
        scratch_shapes=scratch,
        compiler_params=pltpu.CompilerParams(
            collective_id=number, has_side_effects=True, vmem_limit_bytes=64 * 1024 * 1024 - 65536
        ),
        name="relocate",
    )(planes_of(partner, cap), weight_in, weight_out, sent)


def relocate_by_planes(weight_in, weight_out, sent, partner):
    width = lax.axis_size("gy")
    count = crossing_count(partner)
    caps = NARROW + (width,)
    return lax.switch(
        sum(jnp.where(count > cap, 1, 0) for cap in NARROW),
        [functools.partial(relocate_planes, cap, number) for number, cap in enumerate(caps)],
        weight_in,
        weight_out,
        sent,
        partner,
    )


def relocate_flat(weight_in, weight_out, partner):
    devices = lax.axis_size(AXES)
    stacked = jnp.stack([weight_in.reshape(devices, -1), weight_out.reshape(devices, -1)], axis=1)
    pieces = lax.all_to_all(stacked, AXES, split_axis=0, concat_axis=0, tiled=True)
    reordered = jnp.take(pieces, partner, axis=0)
    settled = lax.all_to_all(reordered, AXES, split_axis=0, concat_axis=0, tiled=True)
    return (settled[:, 0].reshape(weight_in.shape), settled[:, 1].reshape(weight_out.shape))


def seated(groups, routes, norm_gain, old_place, seat):
    devices = lax.axis_size(AXES)
    rows, model_width = groups[0].shape
    slots = lax.iota(jnp.int32, devices)
    places = []
    lower = (
        lax.broadcasted_iota(jnp.int32, (rows, rows), 0)
        > lax.broadcasted_iota(jnp.int32, (rows, rows), 1)
    ).astype(jnp.bfloat16)
    for block, names in enumerate(routes):
        member = names == old_place[None, :]
        before = jnp.dot(lower, member.astype(jnp.bfloat16), preferred_element_type=jnp.float32)
        spot = slots[None, :] * seat + block * CAP + before.astype(jnp.int32)
        places.append(jnp.sum(jnp.where(member, spot, 0), axis=1))
    place = jnp.concatenate(places)
    total = devices * seat
    values = jnp.concatenate(groups, axis=0).astype(jnp.float32)
    scaling = lax.rsqrt(jnp.mean(values * values, axis=1, keepdims=True) + epsilon)
    normed = (values * scaling * norm_gain).astype(jnp.bfloat16)
    chosen = (lax.iota(jnp.int32, total)[:, None] == place[None, :]).astype(jnp.bfloat16)
    outgoing = jnp.dot(chosen, normed, preferred_element_type=jnp.float32).astype(jnp.bfloat16)
    return chosen, outgoing.reshape(devices, seat, model_width)


def mixed_back(groups, gates, chosen, returned):
    rows, model_width = groups[0].shape
    values = jnp.concatenate(groups, axis=0).astype(jnp.float32)
    answer = lax.dot_general(
        chosen,
        returned.reshape(-1, model_width),
        (((0,), (0,)), ((), ())),
        preferred_element_type=jnp.float32,
    )
    gate = jnp.concatenate(gates)[:, None]
    mixed = (values + gate * answer).astype(jnp.bfloat16)
    return mixed[:rows], mixed[rows:]


def experts_flat(outgoing, weight_in, weight_out):
    devices, seat, model_width = outgoing.shape
    arrived = lax.all_to_all(outgoing, AXES, split_axis=0, concat_axis=0, tiled=True)
    hidden = jnp.maximum(
        jnp.dot(
            arrived.reshape(devices * seat, model_width),
            weight_in[0],
            preferred_element_type=jnp.float32,
        ),
        0.0,
    ).astype(jnp.bfloat16)
    result = jnp.dot(hidden, weight_out[0], preferred_element_type=jnp.float32).astype(jnp.bfloat16)
    return lax.all_to_all(
        result.reshape(devices, seat, model_width), AXES, split_axis=0, concat_axis=0, tiled=True
    )


def local(
    group_one,
    routes_one,
    gates_one,
    group_two,
    routes_two,
    gates_two,
    norm_gain,
    weight_in,
    weight_out,
    old_place,
    partner,
):
    groups, routes, gates = (group_one, group_two), (routes_one, routes_two), (gates_one, gates_two)
    by_planes = (lax.axis_size("gx"), lax.axis_size("gy")) == (4, 8)
    seat = SEAT if by_planes else 2 * CAP
    chosen, outgoing = seated(groups, routes, norm_gain, old_place, seat)
    if by_planes:
        new_in, new_out, returned = relocate_by_planes(weight_in, weight_out, outgoing, partner)
    else:
        new_in, new_out = relocate_flat(weight_in, weight_out, partner)
        returned = experts_flat(outgoing, weight_in, weight_out)
    first, second = mixed_back(groups, gates, chosen, returned)
    return (first, second, new_in, new_out)


def solution(mesh):
    split = ("gx", "gy")
    rows, flat, cube = P(split, None), P(split), P(split, None, None)
    return jax.shard_map(
        local,
        mesh=mesh,
        in_specs=(rows, rows, flat, rows, rows, flat, P(), cube, cube, P(), P()),
        out_specs=(rows, rows, cube, cube),
        check_vma=False,
    )
```

```python
import functools

import jax
import jax.numpy as jnp
from jax import lax
from jax.experimental import pallas as pl
from jax.experimental.pallas import tpu as pltpu
from jax.sharding import PartitionSpec as P

CAP = 6
AXES = ("gx", "gy")

epsilon = 1e-06


MESH = pl.DeviceIdType.MESH
PARTS = 6
NARROW = (5, 6)
TILE = 256
BLOCKS = 8


def crossing_count(partner):
    planes, width = lax.axis_size("gx"), lax.axis_size("gy")
    labels = lax.iota(jnp.int32, planes * width)
    plane, goal = labels // width, partner // width
    counts = [
        jnp.sum(jnp.where((plane <= cut) & (goal > cut), 1, 0)) for cut in range(planes - 1)
    ]
    return jnp.maximum(jnp.maximum(counts[0], counts[1]), counts[2])


def onehot(hit):
    return jnp.where(hit, 1.0, 0.0).astype(jnp.bfloat16)


def across_lanes(column):
    rows = column.shape[0]
    first = lax.broadcasted_iota(jnp.int32, (rows, rows), 0)
    second = lax.broadcasted_iota(jnp.int32, (rows, rows), 1)
    return jnp.sum(jnp.where(first == second, column, 0.0), axis=0, keepdims=True)


def down_rows(row):
    rows = row.shape[1]
    first = lax.broadcasted_iota(jnp.int32, (rows, rows), 0)
    second = lax.broadcasted_iota(jnp.int32, (rows, rows), 1)
    return jnp.sum(jnp.where(first == second, row, 0.0), axis=1, keepdims=True)


def places_of(routes, old_place, block, rows):
    names = down_rows(routes[...].astype(jnp.float32))
    member = names == old_place[...].astype(jnp.float32)
    lower = onehot(
        lax.broadcasted_iota(jnp.int32, (rows, rows), 0)
        > lax.broadcasted_iota(jnp.int32, (rows, rows), 1)
    )
    before = jnp.dot(lower, onehot(member), preferred_element_type=jnp.float32)
    slot = lax.broadcasted_iota(jnp.int32, member.shape, 1) * (4 * CAP) + block * CAP
    spot = slot.astype(jnp.float32) + before
    return jnp.sum(jnp.where(member, spot, 0.0), axis=1, keepdims=True)


def packets(tab, partner, cap, width):
    gx = lax.axis_index("gx")
    planes = partner.shape[1] // width
    shift = width.bit_length() - 1
    outer = (gx == 0) | (gx == planes - 1)
    goal = partner[...]
    goals = down_rows(goal.astype(jnp.float32)).astype(jnp.int32)
    row = lax.broadcasted_iota(jnp.int32, (goal.shape[1],) * 2, 0)
    column = lax.broadcasted_iota(jnp.int32, (goal.shape[1],) * 2, 1)
    label = lax.broadcasted_iota(jnp.int32, goal.shape, 1)

    def ranks(by):
        same = (row >> by) == (column >> by)
        ahead = same & (row < column) & ((goals >> by) != (row >> by))
        behind = same & (column < row) & ((goal >> by) != (column >> by))
        rank = jnp.sum(jnp.where(ahead, 1.0, 0.0), axis=0, keepdims=True)
        as_column = jnp.sum(jnp.where(behind, 1.0, 0.0), axis=1, keepdims=True)
        partners = jnp.sum(jnp.where(row == goal, as_column, 0.0), axis=0, keepdims=True)
        return rank.astype(jnp.int32), partners.astype(jnp.int32)

    rank_plane, partner_plane = ranks(shift)
    rank_half, partner_half = ranks(shift + 1)
    plane, goal_plane = label >> shift, goal >> shift
    half, goal_half = label >> (shift + 1), goal >> (shift + 1)
    spot, goal_spot = label & (width - 1), goal & (width - 1)
    my_half = gx // 2
    leaves = goal_plane != plane

    def listed(base, count, key, code):
        for i in range(count):
            tab[base + i] = jnp.sum(jnp.where(key == i, code, 0))

    out_of = jnp.where(leaves & (plane == gx), rank_plane, -1)
    over = jnp.where((goal_half != half) & (half == my_half), rank_half, -1)
    first = jnp.where(plane == gx, spot, 16 + rank_plane)
    listed(0, cap, jnp.where(outer, out_of, over), first)
    edge = jnp.where(gx == 1, 0, planes - 1)
    code = jnp.where(goal_plane == gx, goal_spot, 32 + partner_half)
    listed(cap, cap, jnp.where(leaves & (plane == edge), rank_plane, -1), code)
    near = jnp.where(goal_half == my_half, 16 + partner_plane, 32 + partner_half)
    far = jnp.where(outer, 16 + rank_plane, near)
    final = jnp.where(goal_plane == gx, goal_spot, far)
    listed(2 * cap, width, label - gx * width, final)


def relocate_kernel(cap, width, *refs):
    w_in, w_out, partner, group_one, group_two, routes_one, routes_two, gain, old_place = refs[:9]
    o_in, o_out, returned = refs[9:12]
    scr = refs[12:]
    weights, outs = (w_in, w_out), (o_in, o_out)
    chunks = 2 * PARTS
    groups = [scr[i * chunks : (i + 1) * chunks] for i in range(6)]
    own, near, across, ahead, behind, ready = groups
    (own_sem, near_sem, across_sem, spread_sem, ahead_sem, behind_sem, ready_sem, out_sem) = scr[
        6 * chunks : 6 * chunks + 8
    ]
    inbox, sent, arrived_rows, total, tile_in, tile_out, tab, token_sem, tile_sem = scr[6 * chunks + 8 :]
    gx, gy = lax.axis_index("gx"), lax.axis_index("gy")
    planes = 4
    outer = (gx == 0) | (gx == planes - 1)
    inner = jnp.where(gx == 0, 1, 2)
    edge = jnp.where(gx == 1, 0, 3)
    other = jnp.where(gx == 1, 2, 1)

    def rows(c, piece):
        step = weights[c // PARTS].shape[1] // (width * PARTS)
        start = piece * (step * PARTS) + (c % PARTS) * step
        return pl.ds(pl.multiple_of(start, step), step)

    me = gx * width + gy
    peers = []
    for a in range(planes):
        for b in range(width):
            if a or b:
                peers.append((jnp.bitwise_xor(gx, a), jnp.bitwise_xor(gy, b)))

    barrier = pltpu.get_barrier_semaphore()
    for peer in peers:
        pl.semaphore_signal(barrier, inc=1, device_id=peer, device_id_type=MESH)
    pl.semaphore_wait(barrier, len(peers))

    def to_all(source, dest, send_sem, recv_sem):
        for x, y in peers:
            pltpu.make_async_remote_copy(
                src_ref=source.at[x * width + y],
                dst_ref=dest.at[me],
                send_sem=send_sem,
                recv_sem=recv_sem,
                device_id=(x, y),
                device_id_type=MESH,
            ).start()
        pltpu.make_async_copy(source.at[me], dest.at[me], recv_sem).start()

    def all_here(ref, sem):
        pltpu.make_async_copy(ref, ref, sem).wait()

    tiles = w_in.shape[2] // TILE

    def tile_copies(f, slot):
        at = pl.ds(pl.multiple_of(f * TILE, TILE), TILE)
        return (
            pltpu.make_async_copy(w_in.at[0, :, at], tile_in.at[slot], tile_sem.at[0, slot]),
            pltpu.make_async_copy(w_out.at[0, at, :], tile_out.at[slot], tile_sem.at[1, slot]),
        )

    for copy in tile_copies(0, 0):
        copy.start()

    def seats_of(order):
        return order + 2 * CAP * ((order * 5462) >> 16)

    def prepare():
        seats, seat, part = sent.shape
        flat = 0.0
        pairs = ((group_one, routes_one), (group_two, routes_two))
        for block, (group, routes) in enumerate(pairs):
            rows_in = group.shape[0]
            place = across_lanes(places_of(routes, old_place, block, rows_in)).astype(jnp.int32)
            values = group[...].astype(jnp.float32)
            scaling = lax.rsqrt(jnp.mean(values * values, axis=1, keepdims=True) + epsilon)
            normed = (values * scaling * gain[...]).astype(jnp.bfloat16)
            spots = lax.broadcasted_iota(jnp.int32, (seats * seat, rows_in), 0)
            for number in range(2):
                chosen = onehot(spots == place + number * (seat // 2))
                flat += jnp.dot(
                    chosen,
                    normed[:, number * part : (number + 1) * part],
                    preferred_element_type=jnp.float32,
                )
        sent[...] = flat.astype(jnp.bfloat16).reshape(sent.shape)

    def expert():
        all_here(inbox, token_sem.at[1])
        seats, seat, part = inbox.shape
        count = seats * seat // 2
        flat = inbox[...].reshape(2 * count, part)
        for number in range(2):
            spot = seats_of(lax.broadcasted_iota(jnp.int32, (count, 2 * count), 0))
            here = lax.broadcasted_iota(jnp.int32, (count, 2 * count), 1)
            chosen = onehot(here == spot + number * (seat // 2))
            arrived_rows[:, number * part : (number + 1) * part] = jnp.dot(
                chosen, flat, preferred_element_type=jnp.float32
            ).astype(jnp.bfloat16)
        total[...] = jnp.zeros_like(total)

        def one(f, carry):
            slot = f % 2
            for copy in tile_copies(f, slot):
                copy.wait()

            @pl.when(f + 1 < tiles)
            def _():
                for copy in tile_copies(f + 1, 1 - slot):
                    copy.start()

            for m in range(2):
                rows_here = pl.ds(m * (count // 2), count // 2)
                tokens = arrived_rows[rows_here, :]
                hidden = jnp.dot(tokens, tile_in[slot], preferred_element_type=jnp.float32)
                hidden = jnp.maximum(hidden, 0.0).astype(jnp.bfloat16)
                total[rows_here, :] += jnp.dot(
                    hidden, tile_out[slot], preferred_element_type=jnp.float32
                )
            return carry

        lax.fori_loop(0, tiles, one, 0)
        flat = 0.0
        for number in range(2):
            spot = seats_of(lax.broadcasted_iota(jnp.int32, (2 * count, count), 1))
            here = lax.broadcasted_iota(jnp.int32, (2 * count, count), 0)
            chosen = onehot(here == spot + number * (seat // 2))
            result = total[:, number * part : (number + 1) * part].astype(jnp.bfloat16)
            flat += jnp.dot(chosen, result, preferred_element_type=jnp.float32)
        all_here(inbox.at[pl.ds(0, len(peers))], token_sem.at[0])
        sent[...] = flat.astype(jnp.bfloat16).reshape(sent.shape)
        to_all(sent, returned, token_sem.at[2], token_sem.at[3])

    def spread(c):
        weight = weights[c // PARTS]
        for r in range(1, width):
            target = jnp.bitwise_xor(gy, r)
            pltpu.make_async_remote_copy(
                src_ref=weight.at[0, rows(c, target)],
                dst_ref=own[c].at[gy],
                send_sem=spread_sem.at[c],
                recv_sem=own_sem.at[c],
                device_id=(gx, target),
                device_id_type=MESH,
            ).start()
        pltpu.make_async_copy(weight.at[0, rows(c, gy)], own[c].at[gy], own_sem.at[c]).start()

    spread(0)
    prepare()
    to_all(sent, inbox, token_sem.at[0], token_sem.at[1])
    for c in range(1, chunks):
        spread(c)
    packets(tab, partner, cap, width)

    def fill(c, dest, base, count, sources):
        ref = dest[c]
        columns = ref.shape[2]
        tall = ref.shape[1]

        def one(i, carry):
            code = tab[base + i]
            kind, index = code // 16, code % 16
            for part in range(4):
                if tall == 16:
                    at = (slice(None), pl.ds(part * (columns // 4), columns // 4))
                else:
                    at = (pl.ds(part * (tall // 4), tall // 4), slice(None))
                value = None
                for number, source in sources:
                    loaded = source[c][jnp.where(kind == number, index, 0), at[0], at[1]]
                    value = loaded if value is None else jnp.where(kind == number, loaded, value)
                ref[i, at[0], at[1]] = value
            return carry

        lax.fori_loop(0, count, one, 0)

    def send(c, source, target, dest, send_sem, recv_sem):
        pltpu.make_async_remote_copy(
            src_ref=source[c],
            dst_ref=dest[c],
            send_sem=send_sem.at[c],
            recv_sem=recv_sem.at[c],
            device_id=(target, gy),
            device_id_type=MESH,
        ).start()

    def arrived(buffer, sem, c):
        pltpu.make_async_copy(buffer[c], buffer[c], sem.at[c]).wait()

    def collect(c, sources):
        fill(c, ready, 2 * cap, width, sources)
        out = outs[c // PARTS]
        for r in range(1, width):
            target = jnp.bitwise_xor(gy, r)
            pltpu.make_async_remote_copy(
                src_ref=ready[c].at[target],
                dst_ref=out.at[0, rows(c, gy)],
                send_sem=ready_sem.at[c],
                recv_sem=out_sem.at[c // PARTS],
                device_id=(gx, target),
                device_id_type=MESH,
            ).start()
        pltpu.make_async_copy(
            ready[c].at[gy], out.at[0, rows(c, gy)], out_sem.at[c // PARTS]
        ).start()

    @pl.when(outer)
    def _():
        lag = 3
        for t in range(chunks + lag):
            if t < chunks:
                arrived(own, own_sem, t)
                fill(t, ahead, 0, cap, ((0, own),))
                send(t, ahead, inner, near, ahead_sem, near_sem)
            if t == 2:
                expert()
            c = t - lag
            if c >= 0:
                arrived(near, near_sem, c)
                collect(c, ((0, own), (1, near)))

    @pl.when(jnp.logical_not(outer))
    def _():
        for t in range(chunks + 1):
            if t < chunks:
                arrived(own, own_sem, t)
                arrived(near, near_sem, t)
                fill(t, ahead, 0, cap, ((0, own), (1, near)))
                send(t, ahead, other, across, ahead_sem, across_sem)
            if t == 0:
                expert()
            c = t - 1
            if c >= 0:
                arrived(across, across_sem, c)
                fill(c, behind, cap, cap, ((0, own), (2, across)))
                send(c, behind, edge, near, behind_sem, near_sem)
                collect(c, ((0, own), (1, near), (2, across)))

    all_here(returned, token_sem.at[3])
    others = inbox.at[pl.ds(0, len(peers))]
    all_here(others, token_sem.at[2])
    for number in range(2):
        all_here(outs[number], out_sem.at[number])
    for c in range(chunks):
        seven = own[c].at[pl.ds(0, width - 1)]
        pltpu.make_async_copy(seven, seven, spread_sem.at[c]).wait()
        pltpu.make_async_copy(seven, seven, ready_sem.at[c]).wait()
        pltpu.make_async_copy(ahead[c], ahead[c], ahead_sem.at[c]).wait()

    @pl.when(jnp.logical_not(outer))
    def _():
        for c in range(chunks):
            pltpu.make_async_copy(behind[c], behind[c], behind_sem.at[c]).wait()


def relocate_planes(cap, number, weight_in, weight_out, *rest):
    width = lax.axis_size("gy")
    chunks = 2 * PARTS

    def buffers(slots):
        kinds = []
        for weight in (weight_in, weight_out):
            _, tall, columns = weight.shape
            kinds += [pltpu.VMEM((slots, tall // (width * PARTS), columns), weight.dtype)] * PARTS
        return kinds

    scratch = buffers(width) + buffers(cap) * 4 + buffers(width)
    scratch += [pltpu.SemaphoreType.DMA((chunks,))] * 7 + [pltpu.SemaphoreType.DMA((2,))]
    model = weight_in.shape[1]
    devices = lax.axis_size(AXES)
    seats = (devices, 4 * CAP, model // 2)
    scratch += [
        pltpu.VMEM(seats, weight_in.dtype),
        pltpu.VMEM(seats, weight_in.dtype),
        pltpu.VMEM((devices * 2 * CAP, model), weight_in.dtype),
        pltpu.VMEM((devices * 2 * CAP, model), jnp.float32),
        pltpu.VMEM((2, model, TILE), weight_in.dtype),
        pltpu.VMEM((2, TILE, model), weight_in.dtype),
        pltpu.SMEM((2 * cap + width,), jnp.int32),
        pltpu.SemaphoreType.DMA((4,)),
        pltpu.SemaphoreType.DMA((2, 2)),
    ]
    anywhere = pl.BlockSpec(memory_space=pl.ANY)
    return pl.pallas_call(
        lambda *refs: relocate_kernel(cap, width, *refs),
        out_shape=(
            jax.ShapeDtypeStruct(weight_in.shape, weight_in.dtype),
            jax.ShapeDtypeStruct(weight_out.shape, weight_out.dtype),
            jax.ShapeDtypeStruct(seats, weight_in.dtype),
        ),
        in_specs=[anywhere, anywhere] + [pl.BlockSpec(memory_space=pltpu.VMEM)] * len(rest),
        out_specs=(anywhere, anywhere, anywhere),
        scratch_shapes=scratch,
        compiler_params=pltpu.CompilerParams(
            collective_id=number, has_side_effects=True, vmem_limit_bytes=64 * 1024 * 1024 - 65536
        ),
        name="relocate",
    )(weight_in, weight_out, *rest)


def relocate_by_planes(weight_in, weight_out, partner, *tokens):
    width = lax.axis_size("gy")
    count = crossing_count(partner)
    caps = NARROW + (width,)
    return lax.switch(
        sum(jnp.where(count > cap, 1, 0) for cap in NARROW),
        [functools.partial(relocate_planes, cap, number) for number, cap in enumerate(caps)],
        weight_in,
        weight_out,
        partner.reshape(1, -1),
        *tokens,
    )


def finish_kernel(*refs):
    raw_in, raw_out, returned, group_one, group_two, routes_one, routes_two = refs[:7]
    old_place, gates_far = refs[7], refs[8:10]
    new_in, new_out, result_one, result_two = refs[10:14]
    hold_in, hold_out, gates_one, gates_two, read_sem, write_sem, gate_sem = refs[14:]
    gates = [
        pltpu.make_async_copy(gates_far[i], (gates_one, gates_two)[i], gate_sem.at[i])
        for i in range(2)
    ]
    for copy in gates:
        copy.start()
    copies = []
    for raw, hold, new in ((raw_in, hold_in, new_in), (raw_out, hold_out, new_out)):
        tall = raw.shape[1] // BLOCKS
        for k in range(BLOCKS):
            at = pl.ds(k * tall, tall)
            i = len(copies)
            copies.append(
                (
                    pltpu.make_async_copy(raw.at[0, at], hold.at[k], read_sem.at[i]),
                    pltpu.make_async_copy(hold.at[k], new.at[0, at], write_sem.at[i]),
                )
            )
    for read, write in copies:
        read.start()
    ready = iter(copies)

    def pass_on(count):
        for _ in range(count):
            read, write = next(ready)
            read.wait()
            write.start()

    for copy in gates:
        copy.wait()
    pass_on(3)
    seats, seat, part = returned.shape
    flat = returned[...].reshape(seats * seat, part)
    blocks = (
        (group_one, routes_one, gates_one, result_one),
        (group_two, routes_two, gates_two, result_two),
    )
    for block, (group, routes, gates, result) in enumerate(blocks):
        rows = group.shape[0]
        place = places_of(routes, old_place, block, rows).astype(jnp.int32)
        gate = down_rows(gates[...])
        spots = lax.broadcasted_iota(jnp.int32, (rows, seats * seat), 1)
        for number in range(2):
            at = slice(number * part, (number + 1) * part)
            answer = jnp.dot(
                onehot(spots == place + number * (seat // 2)),
                flat,
                preferred_element_type=jnp.float32,
            )
            result[:, at] = (group[:, at].astype(jnp.float32) + gate * answer).astype(result.dtype)
            pass_on(3)
    pass_on(2 * BLOCKS - 15)
    for read, write in copies:
        write.wait()


def finish(raw_in, raw_out, returned, groups, routes, gates, old_place):
    anywhere, local = pl.BlockSpec(memory_space=pl.ANY), pl.BlockSpec(memory_space=pltpu.VMEM)

    def held(raw):
        return pltpu.VMEM((BLOCKS, raw.shape[1] // BLOCKS, raw.shape[2]), raw.dtype)

    new_in, new_out, one, two = pl.pallas_call(
        finish_kernel,
        out_shape=[jax.ShapeDtypeStruct(x.shape, x.dtype) for x in (raw_in, raw_out) + groups],
        in_specs=[anywhere] * 2 + [local] * 6 + [anywhere] * 2,
        out_specs=[anywhere] * 2 + [local] * 2,
        scratch_shapes=[held(raw_in), held(raw_out)]
        + [pltpu.VMEM(gate.shape, gate.dtype) for gate in gates]
        + [pltpu.SemaphoreType.DMA((2 * BLOCKS,))] * 2
        + [pltpu.SemaphoreType.DMA((2,))],
        compiler_params=pltpu.CompilerParams(vmem_limit_bytes=60 * 1024 * 1024),
        name="finish",
    )(raw_in, raw_out, returned, *groups, *routes, old_place, *gates)
    return one, two, new_in, new_out


def relocate_flat(weight_in, weight_out, partner):
    devices = lax.axis_size(AXES)
    stacked = jnp.stack([weight_in.reshape(devices, -1), weight_out.reshape(devices, -1)], axis=1)
    pieces = lax.all_to_all(stacked, AXES, split_axis=0, concat_axis=0, tiled=True)
    reordered = jnp.take(pieces, partner, axis=0)
    settled = lax.all_to_all(reordered, AXES, split_axis=0, concat_axis=0, tiled=True)
    return (settled[:, 0].reshape(weight_in.shape), settled[:, 1].reshape(weight_out.shape))


def seated(groups, routes, norm_gain, old_place, seat):
    devices = lax.axis_size(AXES)
    rows, model_width = groups[0].shape
    slots = lax.iota(jnp.int32, devices)
    places = []
    lower = (
        lax.broadcasted_iota(jnp.int32, (rows, rows), 0)
        > lax.broadcasted_iota(jnp.int32, (rows, rows), 1)
    ).astype(jnp.bfloat16)
    for block, names in enumerate(routes):
        member = names == old_place[None, :]
        before = jnp.dot(lower, member.astype(jnp.bfloat16), preferred_element_type=jnp.float32)
        spot = slots[None, :] * seat + block * CAP + before.astype(jnp.int32)
        places.append(jnp.sum(jnp.where(member, spot, 0), axis=1))
    place = jnp.concatenate(places)
    total = devices * seat
    values = jnp.concatenate(groups, axis=0).astype(jnp.float32)
    scaling = lax.rsqrt(jnp.mean(values * values, axis=1, keepdims=True) + epsilon)
    normed = (values * scaling * norm_gain).astype(jnp.bfloat16)
    chosen = (lax.iota(jnp.int32, total)[:, None] == place[None, :]).astype(jnp.bfloat16)
    outgoing = jnp.dot(chosen, normed, preferred_element_type=jnp.float32).astype(jnp.bfloat16)
    return chosen, outgoing.reshape(devices, seat, model_width)


def mixed_back(groups, gates, chosen, returned):
    rows, model_width = groups[0].shape
    values = jnp.concatenate(groups, axis=0).astype(jnp.float32)
    answer = lax.dot_general(
        chosen,
        returned.reshape(-1, model_width),
        (((0,), (0,)), ((), ())),
        preferred_element_type=jnp.float32,
    )
    gate = jnp.concatenate(gates)[:, None]
    mixed = (values + gate * answer).astype(jnp.bfloat16)
    return mixed[:rows], mixed[rows:]


def experts_flat(outgoing, weight_in, weight_out):
    devices, seat, model_width = outgoing.shape
    arrived = lax.all_to_all(outgoing, AXES, split_axis=0, concat_axis=0, tiled=True)
    hidden = jnp.maximum(
        jnp.dot(
            arrived.reshape(devices * seat, model_width),
            weight_in[0],
            preferred_element_type=jnp.float32,
        ),
        0.0,
    ).astype(jnp.bfloat16)
    result = jnp.dot(hidden, weight_out[0], preferred_element_type=jnp.float32).astype(jnp.bfloat16)
    return lax.all_to_all(
        result.reshape(devices, seat, model_width), AXES, split_axis=0, concat_axis=0, tiled=True
    )


def local(
    group_one,
    routes_one,
    gates_one,
    group_two,
    routes_two,
    gates_two,
    norm_gain,
    weight_in,
    weight_out,
    old_place,
    partner,
):
    groups, routes, gates = (group_one, group_two), (routes_one, routes_two), (gates_one, gates_two)
    by_planes = (lax.axis_size("gx"), lax.axis_size("gy")) == (4, 8)
    if by_planes:
        routes = tuple(x.reshape(1, -1) for x in routes)
        gates = tuple(x.reshape(1, -1) for x in gates)
        holders = old_place.reshape(1, -1)
        raw_in, raw_out, returned = relocate_by_planes(
            weight_in, weight_out, partner, *groups, *routes, norm_gain, holders
        )
        return finish(raw_in, raw_out, returned, groups, routes, gates, holders)
    chosen, outgoing = seated(groups, routes, norm_gain, old_place, 2 * CAP)
    new_in, new_out = relocate_flat(weight_in, weight_out, partner)
    returned = experts_flat(outgoing, weight_in, weight_out)
    first, second = mixed_back(groups, gates, chosen, returned)
    return (first, second, new_in, new_out)


def solution(mesh):
    split = ("gx", "gy")
    rows, flat, cube = P(split, None), P(split), P(split, None, None)
    return jax.shard_map(
        local,
        mesh=mesh,
        in_specs=(rows, rows, flat, rows, rows, flat, P(), cube, cube, P(), P()),
        out_specs=(rows, rows, cube, cube),
        check_vma=False,
    )
```

```python
import functools

import jax
import jax.numpy as jnp
from jax import lax
from jax.experimental import pallas as pl
from jax.experimental.pallas import tpu as pltpu
from jax.sharding import PartitionSpec as P

CAP = 6
AXES = ("gx", "gy")

epsilon = 1e-06


MESH = pl.DeviceIdType.MESH
PARTS = 6
NARROW = (5, 6)
TILE = 256
BLOCKS = 8


def choose_kernel(planes, width, partner, choice):
    shift = width.bit_length() - 1
    counts = [0] * (planes - 1)
    for slot in range(planes * width):
        goal = partner[slot] >> shift
        for cut in range(slot // width, planes - 1):
            counts[cut] += jnp.where(goal > cut, 1, 0)
    count = functools.reduce(jnp.maximum, counts)
    choice[0] = sum(jnp.where(count > cap, 1, 0) for cap in NARROW)


def chosen_form(partner):
    planes, width = lax.axis_size("gx"), lax.axis_size("gy")
    smem = pl.BlockSpec(memory_space=pltpu.SMEM)
    return pl.pallas_call(
        functools.partial(choose_kernel, planes, width),
        out_shape=jax.ShapeDtypeStruct((1,), jnp.int32),
        in_specs=[smem],
        out_specs=smem,
        name="choose",
    )(partner)[0]


def onehot(hit):
    return jnp.where(hit, 1.0, 0.0).astype(jnp.bfloat16)


def across_lanes(column):
    rows = column.shape[0]
    first = lax.broadcasted_iota(jnp.int32, (rows, rows), 0)
    second = lax.broadcasted_iota(jnp.int32, (rows, rows), 1)
    return jnp.sum(jnp.where(first == second, column, 0.0), axis=0, keepdims=True)


def down_rows(row):
    rows = row.shape[1]
    first = lax.broadcasted_iota(jnp.int32, (rows, rows), 0)
    second = lax.broadcasted_iota(jnp.int32, (rows, rows), 1)
    return jnp.sum(jnp.where(first == second, row, 0.0), axis=1, keepdims=True)


def places_of(routes, old_place, block, rows):
    names = down_rows(routes[...].astype(jnp.float32))
    member = names == old_place[...].astype(jnp.float32)
    lower = onehot(
        lax.broadcasted_iota(jnp.int32, (rows, rows), 0)
        > lax.broadcasted_iota(jnp.int32, (rows, rows), 1)
    )
    before = jnp.dot(lower, onehot(member), preferred_element_type=jnp.float32)
    slot = lax.broadcasted_iota(jnp.int32, member.shape, 1) * (4 * CAP) + block * CAP
    spot = slot.astype(jnp.float32) + before
    return jnp.sum(jnp.where(member, spot, 0.0), axis=1, keepdims=True)


def packets(tab, partner, cap, width):
    gx = lax.axis_index("gx")
    planes = partner.shape[1] // width
    shift = width.bit_length() - 1
    outer = (gx == 0) | (gx == planes - 1)
    goal = partner[...]
    goals = down_rows(goal.astype(jnp.float32)).astype(jnp.int32)
    row = lax.broadcasted_iota(jnp.int32, (goal.shape[1],) * 2, 0)
    column = lax.broadcasted_iota(jnp.int32, (goal.shape[1],) * 2, 1)
    label = lax.broadcasted_iota(jnp.int32, goal.shape, 1)

    def ranks(by):
        same = (row >> by) == (column >> by)
        ahead = same & (row < column) & ((goals >> by) != (row >> by))
        behind = same & (column < row) & ((goal >> by) != (column >> by))
        rank = jnp.sum(jnp.where(ahead, 1.0, 0.0), axis=0, keepdims=True)
        as_column = jnp.sum(jnp.where(behind, 1.0, 0.0), axis=1, keepdims=True)
        partners = jnp.sum(jnp.where(row == goal, as_column, 0.0), axis=0, keepdims=True)
        return rank.astype(jnp.int32), partners.astype(jnp.int32)

    rank_plane, partner_plane = ranks(shift)
    rank_half, partner_half = ranks(shift + 1)
    plane, goal_plane = label >> shift, goal >> shift
    half, goal_half = label >> (shift + 1), goal >> (shift + 1)
    spot, goal_spot = label & (width - 1), goal & (width - 1)
    my_half = gx // 2
    leaves = goal_plane != plane

    def listed(base, count, key, code):
        for i in range(count):
            tab[base + i] = jnp.sum(jnp.where(key == i, code, 0))

    out_of = jnp.where(leaves & (plane == gx), rank_plane, -1)
    over = jnp.where((goal_half != half) & (half == my_half), rank_half, -1)
    first = jnp.where(plane == gx, spot, 16 + rank_plane)
    listed(0, cap, jnp.where(outer, out_of, over), first)
    edge = jnp.where(gx == 1, 0, planes - 1)
    code = jnp.where(goal_plane == gx, goal_spot, 32 + partner_half)
    listed(cap, cap, jnp.where(leaves & (plane == edge), rank_plane, -1), code)
    near = jnp.where(goal_half == my_half, 16 + partner_plane, 32 + partner_half)
    far = jnp.where(outer, 16 + rank_plane, near)
    final = jnp.where(goal_plane == gx, goal_spot, far)
    listed(2 * cap, width, label - gx * width, final)


def relocate_kernel(cap, width, *refs):
    w_in, w_out, partner, group_one, group_two, routes_one, routes_two, gain, old_place = refs[:9]
    o_in, o_out, returned = refs[9:12]
    scr = refs[12:]
    weights, outs = (w_in, w_out), (o_in, o_out)
    chunks = 2 * PARTS
    groups = [scr[i * chunks : (i + 1) * chunks] for i in range(6)]
    own, near, across, ahead, behind, ready = groups
    (own_sem, near_sem, across_sem, spread_sem, ahead_sem, behind_sem, ready_sem, out_sem) = scr[
        6 * chunks : 6 * chunks + 8
    ]
    inbox, sent, arrived_rows, total, tile_in, tile_out, tab, token_sem, tile_sem = scr[6 * chunks + 8 :]
    gx, gy = lax.axis_index("gx"), lax.axis_index("gy")
    planes = 4
    outer = (gx == 0) | (gx == planes - 1)
    inner = jnp.where(gx == 0, 1, 2)
    edge = jnp.where(gx == 1, 0, 3)
    other = jnp.where(gx == 1, 2, 1)

    def rows(c, piece):
        step = weights[c // PARTS].shape[1] // (width * PARTS)
        start = piece * (step * PARTS) + (c % PARTS) * step
        return pl.ds(pl.multiple_of(start, step), step)

    me = gx * width + gy
    peers = []
    for a in range(planes):
        for b in range(width):
            if a or b:
                peers.append((jnp.bitwise_xor(gx, a), jnp.bitwise_xor(gy, b)))

    barrier = pltpu.get_barrier_semaphore()
    for peer in peers:
        pl.semaphore_signal(barrier, inc=1, device_id=peer, device_id_type=MESH)
    pl.semaphore_wait(barrier, len(peers))

    def to_all(source, dest, send_sem, recv_sem):
        for x, y in peers:
            pltpu.make_async_remote_copy(
                src_ref=source.at[x * width + y],
                dst_ref=dest.at[me],
                send_sem=send_sem,
                recv_sem=recv_sem,
                device_id=(x, y),
                device_id_type=MESH,
            ).start()
        pltpu.make_async_copy(source.at[me], dest.at[me], recv_sem).start()

    def all_here(ref, sem):
        pltpu.make_async_copy(ref, ref, sem).wait()

    tiles = w_in.shape[2] // TILE

    def tile_copies(f, slot):
        at = pl.ds(pl.multiple_of(f * TILE, TILE), TILE)
        return (
            pltpu.make_async_copy(w_in.at[0, :, at], tile_in.at[slot], tile_sem.at[0, slot]),
            pltpu.make_async_copy(w_out.at[0, at, :], tile_out.at[slot], tile_sem.at[1, slot]),
        )

    for copy in tile_copies(0, 0):
        copy.start()

    def seats_of(order):
        return order + 2 * CAP * ((order * 5462) >> 16)

    def prepare():
        seats, seat, part = sent.shape
        flat = 0.0
        pairs = ((group_one, routes_one), (group_two, routes_two))
        for block, (group, routes) in enumerate(pairs):
            rows_in = group.shape[0]
            place = across_lanes(places_of(routes, old_place, block, rows_in)).astype(jnp.int32)
            values = group[...].astype(jnp.float32)
            scaling = lax.rsqrt(jnp.mean(values * values, axis=1, keepdims=True) + epsilon)
            normed = (values * scaling * gain[...]).astype(jnp.bfloat16)
            spots = lax.broadcasted_iota(jnp.int32, (seats * seat, rows_in), 0)
            for number in range(2):
                chosen = onehot(spots == place + number * (seat // 2))
                flat += jnp.dot(
                    chosen,
                    normed[:, number * part : (number + 1) * part],
                    preferred_element_type=jnp.float32,
                )
        sent[...] = flat.astype(jnp.bfloat16).reshape(sent.shape)

    def expert():
        all_here(inbox, token_sem.at[1])
        seats, seat, part = inbox.shape
        count = seats * seat // 2
        flat = inbox[...].reshape(2 * count, part)
        for number in range(2):
            spot = seats_of(lax.broadcasted_iota(jnp.int32, (count, 2 * count), 0))
            here = lax.broadcasted_iota(jnp.int32, (count, 2 * count), 1)
            chosen = onehot(here == spot + number * (seat // 2))
            arrived_rows[:, number * part : (number + 1) * part] = jnp.dot(
                chosen, flat, preferred_element_type=jnp.float32
            ).astype(jnp.bfloat16)
        total[...] = jnp.zeros_like(total)

        def one(f, carry):
            slot = f % 2
            for copy in tile_copies(f, slot):
                copy.wait()

            @pl.when(f + 1 < tiles)
            def _():
                for copy in tile_copies(f + 1, 1 - slot):
                    copy.start()

            for m in range(2):
                rows_here = pl.ds(m * (count // 2), count // 2)
                tokens = arrived_rows[rows_here, :]
                hidden = jnp.dot(tokens, tile_in[slot], preferred_element_type=jnp.float32)
                hidden = jnp.maximum(hidden, 0.0).astype(jnp.bfloat16)
                total[rows_here, :] += jnp.dot(
                    hidden, tile_out[slot], preferred_element_type=jnp.float32
                )
            return carry

        lax.fori_loop(0, tiles, one, 0)
        flat = 0.0
        for number in range(2):
            spot = seats_of(lax.broadcasted_iota(jnp.int32, (2 * count, count), 1))
            here = lax.broadcasted_iota(jnp.int32, (2 * count, count), 0)
            chosen = onehot(here == spot + number * (seat // 2))
            result = total[:, number * part : (number + 1) * part].astype(jnp.bfloat16)
            flat += jnp.dot(chosen, result, preferred_element_type=jnp.float32)
        all_here(inbox.at[pl.ds(0, len(peers))], token_sem.at[0])
        sent[...] = flat.astype(jnp.bfloat16).reshape(sent.shape)
        to_all(sent, returned, token_sem.at[2], token_sem.at[3])

    def spread(c):
        weight = weights[c // PARTS]
        for r in range(1, width):
            target = jnp.bitwise_xor(gy, r)
            pltpu.make_async_remote_copy(
                src_ref=weight.at[0, rows(c, target)],
                dst_ref=own[c].at[gy],
                send_sem=spread_sem.at[c],
                recv_sem=own_sem.at[c],
                device_id=(gx, target),
                device_id_type=MESH,
            ).start()
        pltpu.make_async_copy(weight.at[0, rows(c, gy)], own[c].at[gy], own_sem.at[c]).start()

    spread(0)
    spread(1)
    prepare()
    to_all(sent, inbox, token_sem.at[0], token_sem.at[1])
    for c in range(2, chunks):
        spread(c)
    packets(tab, partner, cap, width)

    def fill(c, dest, base, count, sources):
        ref = dest[c]
        columns = ref.shape[2]
        tall = ref.shape[1]

        def one(i, carry):
            code = tab[base + i]
            kind, index = code // 16, code % 16
            for part in range(4):
                if tall == 16:
                    at = (slice(None), pl.ds(part * (columns // 4), columns // 4))
                else:
                    at = (pl.ds(part * (tall // 4), tall // 4), slice(None))
                value = None
                for number, source in sources:
                    loaded = source[c][jnp.where(kind == number, index, 0), at[0], at[1]]
                    value = loaded if value is None else jnp.where(kind == number, loaded, value)
                ref[i, at[0], at[1]] = value
            return carry

        lax.fori_loop(0, count, one, 0)

    def send(c, source, target, dest, send_sem, recv_sem):
        pltpu.make_async_remote_copy(
            src_ref=source[c],
            dst_ref=dest[c],
            send_sem=send_sem.at[c],
            recv_sem=recv_sem.at[c],
            device_id=(target, gy),
            device_id_type=MESH,
        ).start()

    def arrived(buffer, sem, c):
        pltpu.make_async_copy(buffer[c], buffer[c], sem.at[c]).wait()

    def collect(c, sources):
        fill(c, ready, 2 * cap, width, sources)
        out = outs[c // PARTS]
        for r in range(1, width):
            target = jnp.bitwise_xor(gy, r)
            pltpu.make_async_remote_copy(
                src_ref=ready[c].at[target],
                dst_ref=out.at[0, rows(c, gy)],
                send_sem=ready_sem.at[c],
                recv_sem=out_sem.at[c // PARTS],
                device_id=(gx, target),
                device_id_type=MESH,
            ).start()
        pltpu.make_async_copy(
            ready[c].at[gy], out.at[0, rows(c, gy)], out_sem.at[c // PARTS]
        ).start()

    @pl.when(outer)
    def _():
        lag = 3
        for t in range(chunks + lag):
            if t < chunks:
                arrived(own, own_sem, t)
                fill(t, ahead, 0, cap, ((0, own),))
                send(t, ahead, inner, near, ahead_sem, near_sem)
            if t == 2:
                expert()
            c = t - lag
            if c >= 0:
                arrived(near, near_sem, c)
                collect(c, ((0, own), (1, near)))

    @pl.when(jnp.logical_not(outer))
    def _():
        for t in range(chunks + 1):
            if t < chunks:
                arrived(own, own_sem, t)
                arrived(near, near_sem, t)
                fill(t, ahead, 0, cap, ((0, own), (1, near)))
                send(t, ahead, other, across, ahead_sem, across_sem)
            if t == 0:
                expert()
            c = t - 1
            if c >= 0:
                arrived(across, across_sem, c)
                fill(c, behind, cap, cap, ((0, own), (2, across)))
                send(c, behind, edge, near, behind_sem, near_sem)
                collect(c, ((0, own), (1, near), (2, across)))

    all_here(returned, token_sem.at[3])
    others = inbox.at[pl.ds(0, len(peers))]
    all_here(others, token_sem.at[2])
    for number in range(2):
        all_here(outs[number], out_sem.at[number])
    for c in range(chunks):
        seven = own[c].at[pl.ds(0, width - 1)]
        pltpu.make_async_copy(seven, seven, spread_sem.at[c]).wait()
        pltpu.make_async_copy(seven, seven, ready_sem.at[c]).wait()
        pltpu.make_async_copy(ahead[c], ahead[c], ahead_sem.at[c]).wait()

    @pl.when(jnp.logical_not(outer))
    def _():
        for c in range(chunks):
            pltpu.make_async_copy(behind[c], behind[c], behind_sem.at[c]).wait()


def relocate_planes(cap, number, weight_in, weight_out, *rest):
    width = lax.axis_size("gy")
    chunks = 2 * PARTS

    def buffers(slots):
        kinds = []
        for weight in (weight_in, weight_out):
            _, tall, columns = weight.shape
            kinds += [pltpu.VMEM((slots, tall // (width * PARTS), columns), weight.dtype)] * PARTS
        return kinds

    scratch = buffers(width) + buffers(cap) * 4 + buffers(width)
    scratch += [pltpu.SemaphoreType.DMA((chunks,))] * 7 + [pltpu.SemaphoreType.DMA((2,))]
    model = weight_in.shape[1]
    devices = lax.axis_size(AXES)
    seats = (devices, 4 * CAP, model // 2)
    scratch += [
        pltpu.VMEM(seats, weight_in.dtype),
        pltpu.VMEM(seats, weight_in.dtype),
        pltpu.VMEM((devices * 2 * CAP, model), weight_in.dtype),
        pltpu.VMEM((devices * 2 * CAP, model), jnp.float32),
        pltpu.VMEM((2, model, TILE), weight_in.dtype),
        pltpu.VMEM((2, TILE, model), weight_in.dtype),
        pltpu.SMEM((2 * cap + width,), jnp.int32),
        pltpu.SemaphoreType.DMA((4,)),
        pltpu.SemaphoreType.DMA((2, 2)),
    ]
    anywhere = pl.BlockSpec(memory_space=pl.ANY)
    return pl.pallas_call(
        lambda *refs: relocate_kernel(cap, width, *refs),
        out_shape=(
            jax.ShapeDtypeStruct(weight_in.shape, weight_in.dtype),
            jax.ShapeDtypeStruct(weight_out.shape, weight_out.dtype),
            jax.ShapeDtypeStruct(seats, weight_in.dtype),
        ),
        in_specs=[anywhere, anywhere] + [pl.BlockSpec(memory_space=pltpu.VMEM)] * len(rest),
        out_specs=(anywhere, anywhere, anywhere),
        scratch_shapes=scratch,
        compiler_params=pltpu.CompilerParams(
            collective_id=number, has_side_effects=True, vmem_limit_bytes=64 * 1024 * 1024 - 65536
        ),
        name="relocate",
    )(weight_in, weight_out, *rest)


def relocate_by_planes(weight_in, weight_out, partner, *tokens):
    width = lax.axis_size("gy")
    caps = NARROW + (width,)
    return lax.switch(
        chosen_form(partner),
        [functools.partial(relocate_planes, cap, number) for number, cap in enumerate(caps)],
        weight_in,
        weight_out,
        partner.reshape(1, -1),
        *tokens,
    )


def finish_kernel(*refs):
    raw_in, raw_out, returned, group_one, group_two, routes_one, routes_two = refs[:7]
    old_place, gates_far = refs[7], refs[8:10]
    new_in, new_out, result_one, result_two = refs[10:14]
    hold_in, hold_out, gates_one, gates_two, read_sem, write_sem, gate_sem = refs[14:]
    gates = [
        pltpu.make_async_copy(gates_far[i], (gates_one, gates_two)[i], gate_sem.at[i])
        for i in range(2)
    ]
    for copy in gates:
        copy.start()
    copies = []
    for raw, hold, new in ((raw_in, hold_in, new_in), (raw_out, hold_out, new_out)):
        tall = raw.shape[1] // BLOCKS
        for k in range(BLOCKS):
            at = pl.ds(k * tall, tall)
            i = len(copies)
            copies.append(
                (
                    pltpu.make_async_copy(raw.at[0, at], hold.at[k], read_sem.at[i]),
                    pltpu.make_async_copy(hold.at[k], new.at[0, at], write_sem.at[i]),
                )
            )
    for read, write in copies:
        read.start()
    ready = iter(copies)

    def pass_on(count):
        for _ in range(count):
            read, write = next(ready)
            read.wait()
            write.start()

    for copy in gates:
        copy.wait()
    pass_on(3)
    seats, seat, part = returned.shape
    flat = returned[...].reshape(seats * seat, part)
    blocks = (
        (group_one, routes_one, gates_one, result_one),
        (group_two, routes_two, gates_two, result_two),
    )
    for block, (group, routes, gates, result) in enumerate(blocks):
        rows = group.shape[0]
        place = places_of(routes, old_place, block, rows).astype(jnp.int32)
        gate = down_rows(gates[...])
        spots = lax.broadcasted_iota(jnp.int32, (rows, seats * seat), 1)
        for number in range(2):
            at = slice(number * part, (number + 1) * part)
            answer = jnp.dot(
                onehot(spots == place + number * (seat // 2)),
                flat,
                preferred_element_type=jnp.float32,
            )
            result[:, at] = (group[:, at].astype(jnp.float32) + gate * answer).astype(result.dtype)
            pass_on(3)
    pass_on(2 * BLOCKS - 15)
    for read, write in copies:
        write.wait()


def finish(raw_in, raw_out, returned, groups, routes, gates, old_place):
    anywhere, local = pl.BlockSpec(memory_space=pl.ANY), pl.BlockSpec(memory_space=pltpu.VMEM)

    def held(raw):
        return pltpu.VMEM((BLOCKS, raw.shape[1] // BLOCKS, raw.shape[2]), raw.dtype)

    new_in, new_out, one, two = pl.pallas_call(
        finish_kernel,
        out_shape=[jax.ShapeDtypeStruct(x.shape, x.dtype) for x in (raw_in, raw_out) + groups],
        in_specs=[anywhere] * 2 + [local] * 6 + [anywhere] * 2,
        out_specs=[anywhere] * 2 + [local] * 2,
        scratch_shapes=[held(raw_in), held(raw_out)]
        + [pltpu.VMEM(gate.shape, gate.dtype) for gate in gates]
        + [pltpu.SemaphoreType.DMA((2 * BLOCKS,))] * 2
        + [pltpu.SemaphoreType.DMA((2,))],
        compiler_params=pltpu.CompilerParams(vmem_limit_bytes=60 * 1024 * 1024),
        name="finish",
    )(raw_in, raw_out, returned, *groups, *routes, old_place, *gates)
    return one, two, new_in, new_out


def relocate_flat(weight_in, weight_out, partner):
    devices = lax.axis_size(AXES)
    stacked = jnp.stack([weight_in.reshape(devices, -1), weight_out.reshape(devices, -1)], axis=1)
    pieces = lax.all_to_all(stacked, AXES, split_axis=0, concat_axis=0, tiled=True)
    reordered = jnp.take(pieces, partner, axis=0)
    settled = lax.all_to_all(reordered, AXES, split_axis=0, concat_axis=0, tiled=True)
    return (settled[:, 0].reshape(weight_in.shape), settled[:, 1].reshape(weight_out.shape))


def seated(groups, routes, norm_gain, old_place, seat):
    devices = lax.axis_size(AXES)
    rows, model_width = groups[0].shape
    slots = lax.iota(jnp.int32, devices)
    places = []
    lower = (
        lax.broadcasted_iota(jnp.int32, (rows, rows), 0)
        > lax.broadcasted_iota(jnp.int32, (rows, rows), 1)
    ).astype(jnp.bfloat16)
    for block, names in enumerate(routes):
        member = names == old_place[None, :]
        before = jnp.dot(lower, member.astype(jnp.bfloat16), preferred_element_type=jnp.float32)
        spot = slots[None, :] * seat + block * CAP + before.astype(jnp.int32)
        places.append(jnp.sum(jnp.where(member, spot, 0), axis=1))
    place = jnp.concatenate(places)
    total = devices * seat
    values = jnp.concatenate(groups, axis=0).astype(jnp.float32)
    scaling = lax.rsqrt(jnp.mean(values * values, axis=1, keepdims=True) + epsilon)
    normed = (values * scaling * norm_gain).astype(jnp.bfloat16)
    chosen = (lax.iota(jnp.int32, total)[:, None] == place[None, :]).astype(jnp.bfloat16)
    outgoing = jnp.dot(chosen, normed, preferred_element_type=jnp.float32).astype(jnp.bfloat16)
    return chosen, outgoing.reshape(devices, seat, model_width)


def mixed_back(groups, gates, chosen, returned):
    rows, model_width = groups[0].shape
    values = jnp.concatenate(groups, axis=0).astype(jnp.float32)
    answer = lax.dot_general(
        chosen,
        returned.reshape(-1, model_width),
        (((0,), (0,)), ((), ())),
        preferred_element_type=jnp.float32,
    )
    gate = jnp.concatenate(gates)[:, None]
    mixed = (values + gate * answer).astype(jnp.bfloat16)
    return mixed[:rows], mixed[rows:]


def experts_flat(outgoing, weight_in, weight_out):
    devices, seat, model_width = outgoing.shape
    arrived = lax.all_to_all(outgoing, AXES, split_axis=0, concat_axis=0, tiled=True)
    hidden = jnp.maximum(
        jnp.dot(
            arrived.reshape(devices * seat, model_width),
            weight_in[0],
            preferred_element_type=jnp.float32,
        ),
        0.0,
    ).astype(jnp.bfloat16)
    result = jnp.dot(hidden, weight_out[0], preferred_element_type=jnp.float32).astype(jnp.bfloat16)
    return lax.all_to_all(
        result.reshape(devices, seat, model_width), AXES, split_axis=0, concat_axis=0, tiled=True
    )


def local(
    group_one,
    routes_one,
    gates_one,
    group_two,
    routes_two,
    gates_two,
    norm_gain,
    weight_in,
    weight_out,
    old_place,
    partner,
):
    groups, routes, gates = (group_one, group_two), (routes_one, routes_two), (gates_one, gates_two)
    by_planes = (lax.axis_size("gx"), lax.axis_size("gy")) == (4, 8)
    if by_planes:
        routes = tuple(x.reshape(1, -1) for x in routes)
        gates = tuple(x.reshape(1, -1) for x in gates)
        holders = old_place.reshape(1, -1)
        raw_in, raw_out, returned = relocate_by_planes(
            weight_in, weight_out, partner, *groups, *routes, norm_gain, holders
        )
        return finish(raw_in, raw_out, returned, groups, routes, gates, holders)
    chosen, outgoing = seated(groups, routes, norm_gain, old_place, 2 * CAP)
    new_in, new_out = relocate_flat(weight_in, weight_out, partner)
    returned = experts_flat(outgoing, weight_in, weight_out)
    first, second = mixed_back(groups, gates, chosen, returned)
    return (first, second, new_in, new_out)


def solution(mesh):
    split = ("gx", "gy")
    rows, flat, cube = P(split, None), P(split), P(split, None, None)
    return jax.shard_map(
        local,
        mesh=mesh,
        in_specs=(rows, rows, flat, rows, rows, flat, P(), cube, cube, P(), P()),
        out_specs=(rows, rows, cube, cube),
        check_vma=False,
    )
```
